32 devices in a mesh: grp: 2 (over x), wide: 16 (over z, y, core).
Axes of the slice: x: 2, y: 2, z: 4, core: 2. Of those that a mesh axis runs over, the one named last changes fastest.
Arguments:
- x_pool: bfloat16 [16384, 7168], P(('grp', 'wide')), may hold values from -6 to 6
- token_ids: int32 [4096], P(('grp', 'wide')), may hold values from 0 to 16383, as said below
- cotangent: bfloat16 [4096, 7168], P(('grp', 'wide')), may hold values from -6 to 6
- gate_up: bfloat16 [2, 1024, 7168], P(None, 'wide', 'grp'), may hold values from -0.0625 to 0.0625
- down_weight: bfloat16 [1024, 7168], P('wide', 'grp'), may hold values from -0.1875 to 0.1875
- loss_exponent: int32 [1], replicated, may hold values from 3 to 9
Outputs:
- grad_gate_up: bfloat16 [2, 1024, 7168], P(None, 'wide', 'grp')
- grad_down: bfloat16 [1024, 7168], P('wide', 'grp')
The draws below stay inside these ranges and needn't reach their ends.
Inputs may be any that keep to these rules, and one draw needn't show every extreme that they name: The 128 ids in aligned block b of token_ids name rows b * 512 to (b + 1) * 512 - 1 of x_pool.
All inputs are finite; a program needn't handle non-finite values.
Results may differ from the reference program's by a relative error of at most 0.014.
Values may be sent and summed in bfloat16 or wider, within the bound.
No kernel may reach another device: no remote copies, remote signals or barrier semaphores. Data moves between devices by JAX's collectives and lax.ppermute only.
A program may use at most 192 MiB of HBM per device.

```python
import jax
import jax.numpy as jnp
import numpy as np

D = 7168
F = 1024
BLOCKS = 8
TOK_DEV = 128
POOL_DEV = 512
TOKENS = 4096
POOL = 16384
N_GRP = 2
N_WIDE = 16


def draw_token_ids(key, part):
    offsets = jnp.arange(TOKENS, dtype=jnp.int32) // TOK_DEV * POOL_DEV
    return offsets + jax.random.randint(key, (TOKENS,), 0, POOL_DEV, dtype=jnp.int32)


def shard_levels(key, shape, pieces, smallest, top_value):
    level, own = 1.0, jax.random.fold_in(key, 6)
    for dim, shards_of in pieces:
        heights = jnp.exp(jax.random.uniform(jax.random.fold_in(own, dim), (shards_of,), jnp.float32, smallest / len(pieces), top_value / len(pieces)))
        level = level * jnp.repeat(heights, shape[dim] // shards_of).reshape([-1 if axis == dim else 1 for axis in range(len(shape))])
    return level


def scatter_about(key, extent, width, limit, cuts=(), held_as=jnp.bfloat16):
    gain = shard_levels(key, extent, cuts, -0.22, 0.18) if cuts else 1.0
    drawn = jax.random.normal(key, extent, jnp.float32) * width * gain
    return jnp.minimum(jnp.maximum(drawn, -limit), limit).astype(held_as)


def setup_inputs(seed: int = 0) -> dict:
    key_of = jax.random.split(jax.random.key(seed), 7)
    return {
        "x_pool": scatter_about(key_of[0], (POOL, D), 1.0, 6.0, ((0, 32),)),
        "token_ids": draw_token_ids(jax.random.fold_in(key_of[6], 71), 0),
        "cotangent": scatter_about(key_of[2], (TOKENS, D), 1.0, 6.0, ((0, 32),)),
        "gate_up": scatter_about(key_of[3], (2, F, D), D ** -0.5, 0.0625, ((1, 16), (2, 2))),
        "down_weight": scatter_about(key_of[4], (F, D), F ** -0.5, 0.1875, ((0, 16), (1, 2))),
        "loss_exponent": jax.random.randint(key_of[5], (1,), 3, 10).astype(jnp.int32),
    }


def unscale_of(loss_exponent):
    levels = jnp.arange(16, dtype=jnp.int32)
    powers = jnp.asarray(np.power(0.5, np.arange(16)), dtype=jnp.float32)
    return jnp.sum(jnp.where(levels == loss_exponent[0], powers, jnp.float32(0.0)))


def reference(x_pool, token_ids, cotangent, gate_up, down_weight, loss_exponent):
    picked = jnp.take(x_pool, token_ids, axis=0)
    unscale = unscale_of(loss_exponent)
    gate_act = jnp.dot(picked, gate_up[0].T, preferred_element_type=jnp.float32)
    up_act = jnp.dot(picked, gate_up[1].T, preferred_element_type=jnp.float32)
    delta_hidden = unscale * jnp.dot(cotangent, down_weight.T, preferred_element_type=jnp.float32)
    sigmoid_gate = jax.nn.sigmoid(gate_act)
    hidden = (gate_act * sigmoid_gate * up_act).astype(jnp.bfloat16)
    delta_gate = (delta_hidden * up_act * sigmoid_gate * (1.0 + gate_act * (1.0 - sigmoid_gate))).astype(jnp.bfloat16)
    delta_up = (delta_hidden * gate_act * sigmoid_gate).astype(jnp.bfloat16)
    set_count = N_GRP * (N_WIDE // BLOCKS)
    set_rows = TOKENS // set_count
    total_gate = jnp.zeros((F, D), jnp.float32)
    total_up = jnp.zeros((F, D), jnp.float32)
    total_down = jnp.zeros((F, D), jnp.float32)
    for set_index in range(set_count):
        lower = set_index * set_rows
        upper = lower + set_rows
        rows_in = picked[lower:upper]
        part_gate = jnp.dot(delta_gate[lower:upper].T, rows_in, preferred_element_type=jnp.float32)
        part_up = jnp.dot(delta_up[lower:upper].T, rows_in, preferred_element_type=jnp.float32)
        part_down = unscale * jnp.dot(hidden[lower:upper].T, cotangent[lower:upper], preferred_element_type=jnp.float32)
        total_gate = total_gate + part_gate.astype(jnp.bfloat16).astype(jnp.float32)
        total_up = total_up + part_up.astype(jnp.bfloat16).astype(jnp.float32)
        total_down = total_down + part_down.astype(jnp.bfloat16).astype(jnp.float32)
    grad_gate_up = jnp.stack([total_gate, total_up]).astype(jnp.bfloat16)
    grad_down = total_down.astype(jnp.bfloat16)
    return grad_gate_up, grad_down
```

```python
import jax
import jax.numpy as jnp
import numpy as np
from jax import lax
from jax.sharding import PartitionSpec as P

INNER = 4


def swapped(value, axis, bit):
    mask = 2**bit
    pairs = [(source, source ^ mask) for source in range(lax.axis_size(axis))]
    return lax.ppermute(value, axis, pairs)


def moved(value, step, first, last):
    pairs = [
        (z * INNER + inner, (z + step) * INNER + inner)
        for z in range(first, last)
        for inner in range(INNER)
    ]
    return lax.ppermute(value, "wide", pairs)


def unscale_of(loss_exponent):
    levels = jnp.arange(16, dtype=jnp.int32)
    powers = jnp.asarray(np.power(0.5, np.arange(16)), dtype=jnp.float32)
    return jnp.sum(jnp.where(levels == loss_exponent[0], powers, jnp.float32(0.0)))


def contract_last(left_side, right_side):
    return lax.dot_general(
        left_side, right_side, (((1,), (1,)), ((), ())), preferred_element_type=jnp.float32
    )


def contract_first(left_side, right_side):
    return lax.dot_general(
        left_side, right_side, (((0,), (0,)), ((), ())), preferred_element_type=jnp.float32
    )


def gather_line(tile, line_index, count):
    rights, lefts = [tile], [tile]
    for step in range(1, count):
        rights.append(moved(rights[-1], 1, step - 1, count - 1))
        lefts.append(moved(lefts[-1], -1, 1, count - step + 1))
    return [tile] + [
        jnp.where(line_index >= slot, rights[slot], lefts[count - slot])
        for slot in range(1, count)
    ]


def reduce_line(parts, count):
    right = left = None
    for step in range(1, count):
        right_part = parts[step]
        left_part = parts[count - step]
        if right is not None:
            right_part = (right_part.astype(jnp.float32) + right.astype(jnp.float32)).astype(jnp.bfloat16)
            left_part = (left_part.astype(jnp.float32) + left.astype(jnp.float32)).astype(jnp.bfloat16)
        right = moved(right_part, 1, 0, step)
        left = moved(left_part, -1, count - step, count)
    total = parts[0].astype(jnp.float32)
    if right is not None:
        total = total + right.astype(jnp.float32) + left.astype(jnp.float32)
    return total.astype(jnp.bfloat16)


def share_tokens(values, grp_index):
    half = values.shape[1] // 2
    own = lax.dynamic_slice_in_dim(values, grp_index * half, half, 1)
    other = lax.dynamic_slice_in_dim(values, (1 - grp_index) * half, half, 1)
    from_x = swapped(other, "grp", 0)
    from_y = swapped(own, "wide", 1)
    from_xy = swapped(from_x, "wide", 1)
    near = [own, from_y]
    far = [from_x, from_xy]
    near = near + [swapped(piece, "wide", 0) for piece in near]
    far = far + [swapped(piece, "wide", 0) for piece in far]
    return jnp.concatenate(near + far, axis=0)


def per_device(x_pool, token_ids, cotangent, gate_up, down_weight, loss_exponent):
    wide_count = lax.axis_size("wide")
    outer = wide_count // INNER
    wide_index = lax.axis_index("wide")
    line_index = wide_index // INNER
    grp_index = lax.axis_index("grp")
    device_index = grp_index * wide_count + wide_index
    units = down_weight.shape[0]
    width = down_weight.shape[1]

    weight_tile = jnp.concatenate([gate_up, down_weight[None]], axis=0)
    tiles = gather_line(weight_tile, line_index, outer)

    tokens_grad = share_tokens(cotangent, grp_index)
    local_rows = token_ids - device_index * x_pool.shape[0]
    picked = x_pool.at[local_rows].get(mode="promise_in_bounds")
    tokens_in = share_tokens(picked, grp_index)
    half_rows = tokens_in.shape[0] // 2

    unscale = unscale_of(loss_exponent)
    order = sorted(range(outer), key=lambda slot: 0 if slot == 0 else max(slot, outer - slot))
    cut = outer // 2
    hidden_parts, gate_parts, up_parts = [], [], []
    for slots in (order[:cut], order[cut:]):
        block = len(slots) * units
        gate_up_rows = jnp.concatenate(
            [tiles[slot][kind] for kind in range(2) for slot in slots], axis=0
        )
        down_rows = jnp.concatenate([tiles[slot][2] for slot in slots], axis=0)
        partial = jnp.concatenate(
            [contract_last(tokens_in, gate_up_rows), contract_last(tokens_grad, down_rows)], axis=1
        )
        outgoing = partial.astype(jnp.bfloat16)
        near = swapped(outgoing[half_rows:], "grp", 0)
        far = swapped(outgoing[:half_rows], "grp", 0)
        whole = partial + jnp.concatenate([near, far], axis=0).astype(jnp.float32)
        gate_act = whole[:, :block]
        up_act = whole[:, block : 2 * block]
        delta_hidden = unscale * whole[:, 2 * block :]
        sigmoid_gate = jax.nn.sigmoid(gate_act)
        hidden_parts.append((gate_act * sigmoid_gate * up_act).astype(jnp.bfloat16))
        gate_parts.append(
            (
                delta_hidden * up_act * sigmoid_gate * (1.0 + gate_act * (1.0 - sigmoid_gate))
            ).astype(jnp.bfloat16)
        )
        up_parts.append((delta_hidden * gate_act * sigmoid_gate).astype(jnp.bfloat16))

    def finish(deltas, tokens, scale):
        grad = contract_first(jnp.concatenate(deltas, axis=1), tokens)
        if scale is not None:
            grad = scale * grad
        grad = grad.astype(jnp.bfloat16).reshape(outer, units, width)
        parts = [grad[order.index(slot)] for slot in range(outer)]
        return reduce_line(parts, outer)

    grad_down = finish(hidden_parts, tokens_grad, unscale)
    grad_gate = finish(gate_parts, tokens_in, None)
    grad_up = finish(up_parts, tokens_in, None)
    return jnp.stack([grad_gate, grad_up]), grad_down


def solution(mesh):
    in_specs = (
        P(("grp", "wide"), None),
        P(("grp", "wide")),
        P(("grp", "wide"), None),
        P(None, "wide", "grp"),
        P("wide", "grp"),
        P(),
    )
    out_specs = (P(None, "wide", "grp"), P("wide", "grp"))
    return jax.shard_map(
        per_device, mesh=mesh, in_specs=in_specs, out_specs=out_specs, check_vma=False
    )
```

```python
import jax
import jax.numpy as jnp
import numpy as np
from jax import lax
from jax.sharding import PartitionSpec as P


INNER = 4


def swapped(value, axis, bit):
    mask = 2**bit
    pairs = [(source, source ^ mask) for source in range(lax.axis_size(axis))]
    return lax.ppermute(value, axis, pairs)


def moved(value, step, first, last):
    pairs = [
        (z * INNER + inner, (z + step) * INNER + inner)
        for z in range(first, last)
        for inner in range(INNER)
    ]
    return lax.ppermute(value, "wide", pairs)


def unscale_of(loss_exponent):
    levels = jnp.arange(16, dtype=jnp.int32)
    powers = jnp.asarray(np.power(0.5, np.arange(16)), dtype=jnp.float32)
    return jnp.sum(jnp.where(levels == loss_exponent[0], powers, jnp.float32(0.0)))


def contract_last(left_side, right_side):
    return lax.dot_general(
        left_side, right_side, (((1,), (1,)), ((), ())), preferred_element_type=jnp.float32
    )


def contract_first(left_side, right_side):
    return lax.dot_general(
        left_side, right_side, (((0,), (0,)), ((), ())), preferred_element_type=jnp.float32
    )


def gather_line(tile, line_index, count):
    rights, lefts = [tile], [tile]
    for step in range(1, count):
        rights.append(moved(rights[-1], 1, step - 1, count - 1))
        lefts.append(moved(lefts[-1], -1, 1, count - step + 1))
    tiles = [tile] + [
        jnp.where(line_index >= slot, rights[slot], lefts[count - slot])
        for slot in range(1, count)
    ]
    return tiles, rights[2:3] + lefts[2:3]


def summed(*terms):
    total = terms[0].astype(jnp.float32)
    for term in terms[1:]:
        if term is not None:
            total = total + term.astype(jnp.float32)
    return total.astype(jnp.bfloat16)


def reduce_line(parts, early, count):
    right = left = None
    for step in range(1, count):
        ahead, behind = parts[step], parts[count - step]
        if right is not None and step in early and count - step in early:
            first_right = moved(ahead, 1, 0, 1)
            first_left = moved(behind, -1, count - 1, count)
            right = summed(moved(summed(ahead, right), 1, 1, step), first_right)
            left = summed(moved(summed(behind, left), -1, count - step, count - 1), first_left)
        else:
            right = moved(summed(ahead, right), 1, 0, step)
            left = moved(summed(behind, left), -1, count - step, count)
    return summed(parts[0], right, left)


def share_tokens(values, grp_index, waited):
    half = values.shape[1] // 2
    own = lax.dynamic_slice_in_dim(values, grp_index * half, half, 1)
    other = lax.dynamic_slice_in_dim(values, (1 - grp_index) * half, half, 1)
    from_x = swapped(other, "grp", 0)
    from_y = swapped(own, "wide", 1)
    from_xy = swapped(from_x, "wide", 1)
    core_own = swapped(own, "wide", 0)
    core_x = swapped(from_x, "wide", 0)
    core_y = swapped(from_y, "wide", 0)
    from_xy = lax.optimization_barrier((from_xy, *waited))[0]
    core_xy = swapped(from_xy, "wide", 0)
    near = [own, from_y, core_own, core_y]
    far = [from_x, from_xy, core_x, core_xy]
    return jnp.concatenate(near, axis=0), jnp.concatenate(far, axis=0)


def gradients_of(x_pool, token_ids, cotangent, gate_up, down_weight, loss_exponent):
    wide_count = lax.axis_size("wide")
    outer = wide_count // INNER
    wide_index = lax.axis_index("wide")
    line_index = wide_index // INNER
    grp_index = lax.axis_index("grp")
    device_index = grp_index * wide_count + wide_index
    units = down_weight.shape[0]
    width = down_weight.shape[1]

    weight_tile = jnp.concatenate([gate_up, down_weight[None]], axis=0)
    tiles, second_step = gather_line(weight_tile, line_index, outer)

    tokens_grad = share_tokens(cotangent, grp_index, second_step)
    local_rows = token_ids - device_index * x_pool.shape[0]
    picked = x_pool.at[local_rows].get(mode="promise_in_bounds")
    tokens_in = share_tokens(picked, grp_index, second_step)

    unscale = unscale_of(loss_exponent)
    order = sorted(range(outer), key=lambda slot: 0 if slot == 0 else max(slot, outer - slot))
    cut = outer // 2
    parts = [[None] * outer for _ in range(3)]
    for slots in (order[:cut], order[cut:]):
        block = len(slots) * units
        gate_up_rows = jnp.concatenate(
            [tiles[slot][kind] for kind in range(2) for slot in slots], axis=0
        )
        down_rows = jnp.concatenate([tiles[slot][2] for slot in slots], axis=0)
        own, arrived = [], []
        for side in range(2):
            pair = (
                contract_last(tokens_in[side], gate_up_rows),
                contract_last(tokens_grad[side], down_rows),
            )
            own.append(pair)
            outgoing = jnp.concatenate(pair, axis=1).astype(jnp.bfloat16)
            arrived.append(swapped(outgoing, "grp", 0))
        deltas = []
        for side in range(2):
            other = arrived[1 - side].astype(jnp.float32)
            gate_act = own[side][0][:, :block] + other[:, :block]
            up_act = own[side][0][:, block:] + other[:, block : 2 * block]
            delta_hidden = unscale * (own[side][1] + other[:, 2 * block :])
            sigmoid_gate = jax.nn.sigmoid(gate_act)
            hidden = gate_act * sigmoid_gate * up_act
            delta_gate = (
                delta_hidden * up_act * sigmoid_gate * (1.0 + gate_act * (1.0 - sigmoid_gate))
            )
            delta_up = delta_hidden * gate_act * sigmoid_gate
            deltas.append([value.astype(jnp.bfloat16) for value in (hidden, delta_gate, delta_up)])
        for kind in range(3):
            sources = tokens_grad if kind == 0 else tokens_in
            grad = contract_first(deltas[0][kind], sources[0])
            grad = grad + contract_first(deltas[1][kind], sources[1])
            if kind == 0:
                grad = unscale * grad
            grad = grad.astype(jnp.bfloat16).reshape(len(slots), units, width)
            for place, slot in enumerate(slots):
                parts[kind][slot] = grad[place]

    grad_down, grad_gate, grad_up = [
        reduce_line(parts[kind], order[:cut], outer) for kind in range(3)
    ]
    return jnp.stack([grad_gate, grad_up]), grad_down


def solution(mesh):
    in_specs = (
        P(("grp", "wide"), None),
        P(("grp", "wide")),
        P(("grp", "wide"), None),
        P(None, "wide", "grp"),
        P("wide", "grp"),
        P(),
    )
    out_specs = (P(None, "wide", "grp"), P("wide", "grp"))
    return jax.shard_map(
        gradients_of, mesh=mesh, in_specs=in_specs, out_specs=out_specs, check_vma=False
    )
```
